32 devices in a mesh: rep: 16 (over z, x, core), tp: 2 (over y).
Axes of the slice: x: 2, y: 2, z: 4, core: 2. Of those that a mesh axis runs over, the one named last changes fastest.
Arguments:
- tokens: bfloat16 [16, 256, 3072], P('rep', 'tp'), may hold values from -100 to 100
- norm_gain: float32 [16, 3072], P('rep'), may hold values from 0.5 to 1.5
- w_query: bfloat16 [16, 3072, 2048], P('rep', None, 'tp'), may hold values from -1 to 1
- key_weight: bfloat16 [16, 3072, 1024], P('rep', None, 'tp'), may hold values from -1 to 1
- value_weight: bfloat16 [16, 3072, 1024], P('rep', None, 'tp'), may hold values from -0.109375 to 0.109375
- attention_gradient: bfloat16 [16, 256, 2048], P('rep', None, 'tp'), may hold values from -6 to 6
- global_fragment: float32 [128, 3072], P('tp'), may hold values from -6 to 6
- momentum: float32 [128, 3072], P('tp'), may hold values from -3 to 3
- local_fragment: bfloat16 [16, 128, 3072], P('rep', 'tp'), may hold values from -6 to 6
Outputs:
- grad_query_w: bfloat16 [16, 3072, 2048], P('rep', None, 'tp')
- grad_key_w: bfloat16 [16, 3072, 1024], P('rep', None, 'tp')
- grad_value_w: bfloat16 [16, 3072, 1024], P('rep', None, 'tp')
- grad_gain: float32 [16, 3072], P('rep')
- grad_tokens: bfloat16 [16, 256, 3072], P('rep', 'tp')
- new_global: float32 [128, 3072], P('tp')
- new_momentum: float32 [128, 3072], P('tp')
The draws below stay inside these ranges and needn't reach their ends.
All inputs are finite; a program needn't handle non-finite values.
Results may differ from the reference program's by a relative error of at most 0.019.
The reference program's roundings to bfloat16 on the way count: a program that leaves them out, or rounds other values in their place, can miss the bound.
Values may be sent and summed in bfloat16 or wider, within the bound.
No kernel may reach another device: no remote copies, remote signals or barrier semaphores. Data moves between devices by JAX's collectives and lax.ppermute only.
A program may use at most 128 MiB of HBM per device.

```python
import math
import jax
import jax.numpy as jnp
from jax import lax

MODEL_WIDTH = 3072
QUERY_HEADS = 16
KEY_VALUE_HEADS = 8
HEAD_SIZE = 128
SEQ = 256
FRAG = 128
N_REP = 16
N_TP = 2


def draw_tokens(key, part):
    col_scale = jnp.exp(jax.random.uniform(jax.random.fold_in(key, 12), (1, 1, MODEL_WIDTH), jnp.float32, math.log(0.5), math.log(2.0)))
    row_scale = jnp.exp(jax.random.uniform(jax.random.fold_in(key, 11), (N_REP, SEQ, 1), jnp.float32, 0.0, math.log(10.0)))
    jitter = jax.random.normal(jax.random.fold_in(key, 13), (N_REP, SEQ, MODEL_WIDTH), jnp.float32)
    result = jitter * col_scale * row_scale
    return jnp.clip(result, -100.0, 100.0).astype(jnp.bfloat16)


def draw_w_query(key, part):
    return (jax.random.normal(jax.random.fold_in(key, 21), (N_REP, MODEL_WIDTH, QUERY_HEADS * HEAD_SIZE), jnp.float32) * MODEL_WIDTH ** (-0.5)).astype(jnp.bfloat16)


def draw_key_weight(key, part):
    return (jax.random.normal(jax.random.fold_in(key, 31), (N_REP, MODEL_WIDTH, KEY_VALUE_HEADS * HEAD_SIZE), jnp.float32) * MODEL_WIDTH ** (-0.5)).astype(jnp.bfloat16)


def levels(own_key, shape, pieces, low, largest):
    level, own = 1.0, jax.random.fold_in(own_key, 6)
    for dim, parts in pieces:
        heights = jnp.exp(jax.random.uniform(jax.random.fold_in(own, dim), (parts,), jnp.float32, low / len(pieces), largest / len(pieces)))
        level = level * jnp.repeat(heights, shape[dim] // parts).reshape([-1 if axis == dim else 1 for axis in range(len(shape))])
    return level


def centred(own_key, shape, spread, reach, cuts=(), kind=jnp.bfloat16):
    array = jax.random.normal(own_key, shape, jnp.float32) * spread
    if len(cuts) > 0:
        array = levels(own_key, shape, cuts, -0.22, 0.18) * array
    return jnp.clip(array, min=-reach, max=reach).astype(kind)


def setup_inputs(seed: int = 0) -> dict:
    seeds = jax.random.split(jax.random.key(seed), 10)
    return {
        "tokens": draw_tokens(jax.random.fold_in(seeds[9], 71), 0),
        "norm_gain": jnp.clip(1.0 + 0.1 * jax.random.normal(seeds[1], (N_REP, MODEL_WIDTH), jnp.float32), 0.5, 1.5),
        "w_query": draw_w_query(jax.random.fold_in(seeds[9], 71), 0),
        "key_weight": draw_key_weight(jax.random.fold_in(seeds[9], 71), 0),
        "value_weight": centred(seeds[4], (N_REP, MODEL_WIDTH, KEY_VALUE_HEADS * HEAD_SIZE), MODEL_WIDTH ** -0.5, 0.109375, ((0, 16), (2, 2))),
        "attention_gradient": centred(seeds[5], (N_REP, SEQ, QUERY_HEADS * HEAD_SIZE), 1.0, 6.0, ((0, 16), (2, 2))),
        "global_fragment": centred(seeds[6], (FRAG, MODEL_WIDTH), 1.0, 6.0, ((0, 2),), jnp.float32),
        "momentum": centred(seeds[7], (FRAG, MODEL_WIDTH), 0.5, 3.0, ((0, 2),), jnp.float32),
        "local_fragment": centred(seeds[8], (N_REP, FRAG, MODEL_WIDTH), 1.0, 6.0, ((0, 16), (1, 2))),
    }


epsilon = 1e-05
rope_base = 500000.0
outer_rate = 0.7
outer_momentum = 0.9

def rope_tables(sequence_length, width):
    middle = width // 2
    frequency = rope_base ** (-2.0 * jnp.arange(middle, dtype=jnp.float32) / width)
    angles = jnp.arange(sequence_length, dtype=jnp.float32)[:, None] * frequency[None, :]
    angles = jnp.concatenate([angles, angles], axis=1)
    return (jnp.cos(angles)[:, None, :], jnp.sin(angles)[:, None, :])

def rotate(vectors, cosine_table, sine_table):
    middle = vectors.shape[-1] // 2
    turned = jnp.concatenate([-vectors[..., middle:], vectors[..., :middle]], axis=-1)
    return vectors * cosine_table + turned * sine_table

def reverse_rotation(gradient, cosine_table, sine_table):
    middle = gradient.shape[-1] // 2
    shifted = gradient * sine_table
    turned = jnp.concatenate([shifted[..., middle:], -shifted[..., :middle]], axis=-1)
    return gradient * cosine_table + turned

def attention_reverse(query_rows, rotated_keys, values_bfloat, grad_out, block_of_rows):
    sequence_length = query_rows.shape[0]
    score_scale = query_rows.shape[-1] ** (-0.5)
    keys_wide = rotated_keys.astype(jnp.float32)
    values_wide = values_bfloat.astype(jnp.float32)

    def one_block(running, block_index):
        acc_key, acc_value = running
        offset = block_index * block_of_rows
        query_block = lax.dynamic_slice_in_dim(query_rows, offset, block_of_rows, 0).astype(jnp.float32)
        grad_block = lax.dynamic_slice_in_dim(grad_out, offset, block_of_rows, 0).astype(jnp.float32)
        scores = jnp.einsum('qgrd,kgd->grqk', query_block, keys_wide) * score_scale
        row_pos = offset + jnp.arange(block_of_rows)
        col_pos = jnp.arange(sequence_length)
        allowed = col_pos[None, :] <= row_pos[:, None]
        scores = jnp.where(allowed, scores, -jnp.inf)
        highest = lax.optimization_barrier(jnp.max(scores, axis=-1, keepdims=True))
        powers = jnp.exp(scores - highest)
        probability = powers / lax.optimization_barrier(jnp.sum(powers, axis=-1, keepdims=True))
        prob_low = lax.optimization_barrier(probability.astype(jnp.bfloat16)).astype(jnp.float32)
        acc_value = acc_value + jnp.einsum('grqk,qgrd->kgd', prob_low, grad_block)
        grad_prob = jnp.einsum('qgrd,kgd->grqk', grad_block, values_wide)
        grad_score = probability * (grad_prob - lax.optimization_barrier(jnp.sum(grad_prob * probability, axis=-1, keepdims=True))) * score_scale
        score_low = lax.optimization_barrier(grad_score.astype(jnp.bfloat16)).astype(jnp.float32)
        grad_query = jnp.einsum('grqk,kgd->qgrd', score_low, keys_wide)
        acc_key = acc_key + jnp.einsum('grqk,qgrd->kgd', score_low, query_block)
        return ((acc_key, acc_value), grad_query)
    initial = jnp.zeros(rotated_keys.shape, jnp.float32)
    (acc_key, acc_value), grad_blocks = lax.scan(one_block, (initial, initial), jnp.arange(sequence_length // block_of_rows))
    grad_query = grad_blocks.reshape(query_rows.shape)
    return (grad_query, acc_key, acc_value)

def replica_grads(items):
    tokens, norm_gains, w_query, key_weight, value_weight, attention_gradient = items
    sequence_length = tokens.shape[0]
    widened_rows = tokens.astype(jnp.float32)
    inverse_norm = lax.rsqrt(lax.optimization_barrier(jnp.mean(widened_rows * widened_rows, axis=-1, keepdims=True)) + epsilon)
    normalized_input = widened_rows * inverse_norm
    normalized = (normalized_input * norm_gains[None, :]).astype(jnp.bfloat16)
    cosine_table, sine_table = rope_tables(sequence_length, HEAD_SIZE)
    query_rows = jnp.dot(normalized, w_query, preferred_element_type=jnp.float32).reshape(sequence_length, QUERY_HEADS, HEAD_SIZE)
    query_rows = rotate(query_rows, cosine_table, sine_table).astype(jnp.bfloat16)
    rotated_keys = jnp.dot(normalized, key_weight, preferred_element_type=jnp.float32).reshape(sequence_length, KEY_VALUE_HEADS, HEAD_SIZE)
    rotated_keys = rotate(rotated_keys, cosine_table, sine_table).astype(jnp.bfloat16)
    values_bfloat = jnp.dot(normalized, value_weight, preferred_element_type=jnp.float32).astype(jnp.bfloat16).reshape(sequence_length, KEY_VALUE_HEADS, HEAD_SIZE)
    replica_group = QUERY_HEADS // KEY_VALUE_HEADS
    block_of_rows = min(512, sequence_length)
    query_input_gradient, key_input_gradient, value_input_gradient = attention_reverse(query_rows.reshape(sequence_length, KEY_VALUE_HEADS, replica_group, HEAD_SIZE), rotated_keys, values_bfloat, attention_gradient.reshape(sequence_length, KEY_VALUE_HEADS, replica_group, HEAD_SIZE), block_of_rows)
    dquery = reverse_rotation(query_input_gradient.reshape(sequence_length, QUERY_HEADS, HEAD_SIZE), cosine_table, sine_table).astype(jnp.bfloat16).reshape(sequence_length, QUERY_HEADS * HEAD_SIZE)
    key_gradient = reverse_rotation(key_input_gradient, cosine_table, sine_table).astype(jnp.bfloat16).reshape(sequence_length, KEY_VALUE_HEADS * HEAD_SIZE)
    value_gradient = value_input_gradient.astype(jnp.bfloat16).reshape(sequence_length, KEY_VALUE_HEADS * HEAD_SIZE)
    contract = (((0,), (0,)), ((), ()))
    grad_wq = lax.dot_general(normalized, dquery, contract, preferred_element_type=jnp.float32).astype(jnp.bfloat16)
    grad_wk = lax.dot_general(normalized, key_gradient, contract, preferred_element_type=jnp.float32).astype(jnp.bfloat16)
    grad_wv = lax.dot_general(normalized, value_gradient, contract, preferred_element_type=jnp.float32).astype(jnp.bfloat16)
    query_cols = QUERY_HEADS * HEAD_SIZE // N_TP
    key_value_columns = KEY_VALUE_HEADS * HEAD_SIZE // N_TP
    back = (((1,), (1,)), ((), ()))
    summed_rows = jnp.zeros((sequence_length, MODEL_WIDTH), jnp.float32)
    for shard_index in range(N_TP):
        qa, qb_end = (shard_index * query_cols, (shard_index + 1) * query_cols)
        ka, kb_end = (shard_index * key_value_columns, (shard_index + 1) * key_value_columns)
        partial_value = lax.dot_general(dquery[:, qa:qb_end], w_query[:, qa:qb_end], back, preferred_element_type=jnp.float32)
        partial_value = partial_value + lax.dot_general(key_gradient[:, ka:kb_end], key_weight[:, ka:kb_end], back, preferred_element_type=jnp.float32)
        partial_value = partial_value + lax.dot_general(value_gradient[:, ka:kb_end], value_weight[:, ka:kb_end], back, preferred_element_type=jnp.float32)
        summed_rows = summed_rows + lax.optimization_barrier(partial_value.astype(jnp.bfloat16)).astype(jnp.float32)
    gains_gradient = lax.optimization_barrier(jnp.sum(summed_rows * normalized_input, axis=0))
    scaled_rows = summed_rows * norm_gains[None, :]
    gradient_rows = inverse_norm * (scaled_rows - normalized_input * lax.optimization_barrier(jnp.mean(scaled_rows * normalized_input, axis=-1, keepdims=True)))
    return (grad_wq, grad_wk, grad_wv, gains_gradient, gradient_rows.astype(jnp.bfloat16))

def reference(tokens, norm_gain, w_query, key_weight, value_weight, attention_gradient, global_fragment, momentum, local_fragment):
    grad_wq, grad_wk, grad_wv, gains_gradient, gradient_rows = lax.map(replica_grads, (tokens, norm_gain, w_query, key_weight, value_weight, attention_gradient))
    delta = global_fragment[None, :, :] - local_fragment.astype(jnp.float32)
    mean_delta = lax.optimization_barrier(jnp.sum(delta, axis=0)) / N_REP
    new_momentum = outer_momentum * momentum + mean_delta
    new_global = global_fragment - outer_rate * (mean_delta + outer_momentum * new_momentum)
    return (grad_wq, grad_wk, grad_wv, gains_gradient, gradient_rows, new_global, new_momentum)
```

```python
import functools

import jax
import jax.numpy as jnp
import numpy as np
from jax import lax
from jax.experimental import pallas as pl
from jax.experimental.pallas import tpu as pltpu
from jax.sharding import PartitionSpec as P


HEAD_SIZE = 128

epsilon = 1e-05
rope_base = 500000.0
outer_rate = 0.7
outer_momentum = 0.9

VMEM = pltpu.VMEM
f32, bf16 = jnp.float32, jnp.bfloat16

MAX_CHUNKS = 2
WEIGHT_ROWS = 768


def whole():
    return pl.BlockSpec(memory_space=VMEM)


def anywhere():
    return pl.BlockSpec(memory_space=pl.ANY)


def far(array):
    return pltpu.with_memory_space_constraint(array, pltpu.HBM)


def smem():
    return pl.BlockSpec(memory_space=pltpu.SMEM)


def params(mib):
    return pltpu.CompilerParams(vmem_limit_bytes=mib << 20)


def cost(flops, nbytes):
    return pl.CostEstimate(flops=int(flops), bytes_accessed=int(nbytes), transcendentals=0)


def rope_tables(length, width):
    middle = width // 2
    frequency = rope_base ** (-2.0 * np.arange(middle) / width)
    angles = np.arange(length)[:, None] * frequency[None, :]
    cosine, sine = np.cos(angles), np.sin(angles)
    tables = (cosine, cosine, -sine, sine)
    return jnp.asarray(np.concatenate(tables, 1).astype(np.float32))


def rope(v, cosine, sine):
    return v * cosine + pltpu.roll(v, v.shape[-1] // 2, 1) * sine


def unrope(v, cosine, sine):
    return v * cosine - pltpu.roll(v, v.shape[-1] // 2, 1) * sine


def chunk_count(width):
    for n in range(MAX_CHUNKS, 1, -1):
        if width % (n * 128) == 0:
            return n
    return 1


def step_size(width, most):
    for n in range(most, 0, -128):
        if width % n == 0:
            return n
    return width


def norm_kernel(x_ref, gain_ref, *outs):
    x = x_ref[...].astype(f32)
    inverse = lax.rsqrt(jnp.mean(x * x, axis=-1, keepdims=True) + epsilon)
    normed = ((x * inverse) * gain_ref[...]).astype(bf16)
    width = outs[0].shape[1]
    for c, out in enumerate(outs):
        out[...] = normed[:, c * width : (c + 1) * width]


def norm(x, gain, chunks):
    rows, width = x.shape
    return pl.pallas_call(
        norm_kernel,
        out_shape=[jax.ShapeDtypeStruct((rows, width // chunks), bf16)] * chunks,
        in_specs=[whole()] * 2,
        out_specs=[whole()] * chunks,
        compiler_params=params(8),
        cost_estimate=cost(1.0e9, x.size * 4),
        name="norm",
    )(far(x), far(gain))


def project(chunk, wq, wk, wv, rows):
    return [jnp.dot(chunk, w[rows, :], preferred_element_type=f32) for w in (wq, wk, wv)]


def finish_projection(parts, tables, out, row):
    rows = tables.shape[0]
    cosine, sine = tables[:, :HEAD_SIZE], tables[:, HEAD_SIZE:]
    at = 0
    for part, turned in zip(parts, (True, True, False)):
        for h in range(part.shape[1] // HEAD_SIZE):
            piece = part[:, h * HEAD_SIZE : (h + 1) * HEAD_SIZE]
            if turned:
                piece = rope(piece, cosine, sine)
            out[pl.ds(row, rows), at : at + HEAD_SIZE] = piece.astype(bf16)
            at += HEAD_SIZE


def keep(chunk, normed_all, row, part, sem):
    rows, width = chunk.shape
    place = normed_all.at[pl.ds(row, rows), pl.ds(part * width, width)]
    copy = pltpu.make_async_copy(chunk, place, sem)
    copy.start()
    return copy


def own_kernel(block, depth, index_ref, tables, *refs):
    chunks = refs[:-11]
    wq, wk, wv, out, normed_all, bq, bk, bv, acc, sems, keep_sems = refs[-11:]
    rows, width = chunks[0].shape
    start = pl.multiple_of(index_ref[0] * rows, rows)
    steps = wq.shape[0] // block
    sources, buffers = (wq, wk, wv), (bq, bk, bv)

    def fetch(s):
        part = pl.ds(s * block, block)
        copies = [
            pltpu.make_async_copy(sources[i].at[part], buffers[i].at[part], sems.at[s * 3 + i])
            for i in range(3)
        ]
        for copy in copies:
            copy.start()
        return copies

    flights = [fetch(s) for s in range(depth)]
    kept = [keep(ref, normed_all, start, c, keep_sems.at[c]) for c, ref in enumerate(chunks)]
    for s in range(steps):
        for copy in flights[s]:
            copy.wait()
        if s + depth < steps:
            flights.append(fetch(s + depth))
        c, at = divmod(s * block, width)
        parts = project(chunks[c][:, at : at + block], bq, bk, bv, slice(s * block, (s + 1) * block))
        at = 0
        for part in parts:
            cols = slice(at, at + part.shape[1])
            if s == 0:
                acc[:, cols] = part
            else:
                acc[:, cols] += part
            at += part.shape[1]
    qc, kc = wq.shape[1], wk.shape[1]
    parts = acc[:, :qc], acc[:, qc : qc + kc], acc[:, qc + kc :]
    finish_projection(parts, tables[pl.ds(start, rows), :], out, 0)
    for copy in kept:
        copy.wait()


def project_own(index, chunks, wq, wk, wv, tables):
    rows, width = chunks[0].shape
    qc, kc = wq.shape[1], wk.shape[1]
    block = step_size(width, 512)
    full = wq.shape[0]
    steps = full // block
    total = qc + 2 * kc
    return pl.pallas_call(
        functools.partial(own_kernel, block, min(3, steps)),
        out_shape=[
            jax.ShapeDtypeStruct((rows, total), bf16),
            jax.ShapeDtypeStruct((tables.shape[0], full), bf16),
        ],
        in_specs=[smem(), whole()] + [whole()] * len(chunks) + [anywhere()] * 3,
        out_specs=[whole(), anywhere()],
        scratch_shapes=[
            VMEM((full, qc), bf16),
            VMEM((full, kc), bf16),
            VMEM((full, kc), bf16),
            VMEM((rows, total), f32),
            pltpu.SemaphoreType.DMA((steps * 3,)),
            pltpu.SemaphoreType.DMA((len(chunks),)),
        ],
        compiler_params=params(20),
        cost_estimate=cost(5e9, full * total * 2),
        name="own_projection",
    )(index, tables, *chunks, *[far(w) for w in (wq, wk, wv)])


def part_kernel(part, row_ref, chunk, wq, wk, wv, *rest):
    out, normed_all, sem = rest[-3:]
    acc_in = rest[0] if len(rest) > 4 else None
    rows, width = chunk.shape
    kept = keep(chunk, normed_all, pl.multiple_of(row_ref[0] * rows, rows), part, sem)
    at = 0
    for value in project(chunk[...], wq, wk, wv, slice(part * width, (part + 1) * width)):
        cols = slice(at, at + value.shape[1])
        out[:, cols] = value if acc_in is None else acc_in[:, cols] + value
        at += value.shape[1]
    kept.wait()


def project_part(owner, chunk, wq, wk, wv, acc, normed_all, part):
    rows, width = chunk.shape
    total = wq.shape[1] + 2 * wk.shape[1]
    extra = [] if acc is None else [acc]
    inputs = 5 + len(extra)
    return pl.pallas_call(
        functools.partial(part_kernel, part),
        out_shape=[
            jax.ShapeDtypeStruct((rows, total), f32),
            jax.ShapeDtypeStruct(normed_all.shape, bf16),
        ],
        in_specs=[smem()] + [whole()] * (4 + len(extra)) + [anywhere()],
        out_specs=[whole(), anywhere()],
        input_output_aliases={inputs: 1},
        scratch_shapes=[pltpu.SemaphoreType.DMA],
        compiler_params=params(20),
        cost_estimate=cost(2 * rows * width * total, width * total * 2),
        name="part_projection",
    )(owner, chunk, wq, wk, wv, *extra, far(normed_all))


def attention(all_rows, grad_out, tables, out, qc, kc, block):
    length = all_rows.shape[0]
    group = qc // kc
    scale = HEAD_SIZE ** (-0.5)
    nt = (((1,), (1,)), ((), ()))
    tn = (((0,), (0,)), ((), ()))
    key = lax.broadcasted_iota(jnp.int32, (block, block), 0)
    query = lax.broadcasted_iota(jnp.int32, (block, block), 1)
    allowed = jnp.concatenate([key <= query] * group, 1)
    blocks = length // block
    for g in range(kc // HEAD_SIZE):
        kcols = slice(qc + g * HEAD_SIZE, qc + (g + 1) * HEAD_SIZE)
        vcols = slice(qc + kc + g * HEAD_SIZE, qc + kc + (g + 1) * HEAD_SIZE)
        dk = [None] * blocks
        dv = [None] * blocks
        for a in range(blocks):
            rows = slice(a * block, (a + 1) * block)
            keys = (a + 1) * block
            head = lambda r: slice((g * group + r) * HEAD_SIZE, (g * group + r + 1) * HEAD_SIZE)
            q = jnp.concatenate([all_rows[rows, head(r)] for r in range(group)], 0)
            do = jnp.concatenate([grad_out[rows, head(r)] for r in range(group)], 0)
            k = all_rows[:keys, kcols]
            v = all_rows[:keys, vcols]
            s = lax.dot_general(k, q, nt, preferred_element_type=f32) * scale
            corner = jnp.where(allowed, s[keys - block :], -jnp.inf)
            s = corner if a == 0 else jnp.concatenate([s[: keys - block], corner], 0)
            gprob = lax.dot_general(v, do, nt, preferred_element_type=f32)
            powers = jnp.exp(s - jnp.max(s, axis=0, keepdims=True))
            prob = powers * (1.0 / jnp.sum(powers, axis=0, keepdims=True))
            inner = jnp.sum(gprob * prob, axis=0, keepdims=True)
            low = prob.astype(bf16)
            ds = (prob * (gprob - inner) * scale).astype(bf16)
            part_v = jnp.dot(low, do, preferred_element_type=f32)
            part_k = jnp.dot(ds, q, preferred_element_type=f32)
            dq = lax.dot_general(k, ds, tn, preferred_element_type=f32).T
            for b in range(a + 1):
                piece = slice(b * block, (b + 1) * block)
                dv[b] = part_v[piece] if dv[b] is None else dv[b] + part_v[piece]
                dk[b] = part_k[piece] if dk[b] is None else dk[b] + part_k[piece]
            cosine, sine = tables[rows, :HEAD_SIZE], tables[rows, HEAD_SIZE:]
            for r in range(group):
                piece = unrope(dq[r * block : (r + 1) * block], cosine, sine)
                out[rows, head(r)] = piece.astype(bf16)
        for b in range(blocks):
            rows = slice(b * block, (b + 1) * block)
            cosine, sine = tables[rows, :HEAD_SIZE], tables[rows, HEAD_SIZE:]
            out[rows, kcols] = unrope(dk[b], cosine, sine).astype(bf16)
            out[rows, vcols] = dv[b].astype(bf16)


def last_kernel(part, others, index_ref, chunk, wq, wk, wv, *rest):
    acc_in = rest[0] if len(rest) > others + 7 else None
    ready = rest[-(others + 7) : -7]
    grad_out, tables, _, out, normed_all, all_rows, sem = rest[-7:]
    rows, width = chunk.shape
    qc, kc = wq.shape[1], wk.shape[1]
    n = others + 1
    start = pl.multiple_of(lax.rem(index_ref[0] + 1, n) * rows, rows)
    kept = keep(chunk, normed_all, start, part, sem)
    for d, ref in enumerate(ready):
        owner = lax.rem(index_ref[0] + (n - d), n)
        all_rows[pl.ds(pl.multiple_of(owner * rows, rows), rows), :] = ref[...]
    parts = project(chunk[...], wq, wk, wv, slice(part * width, (part + 1) * width))
    if acc_in is not None:
        before = acc_in[:, :qc], acc_in[:, qc : qc + kc], acc_in[:, qc + kc :]
        parts = [b + p for b, p in zip(before, parts)]
    finish_projection(parts, tables[pl.ds(start, rows), :], all_rows, start)
    attention(all_rows, grad_out, tables, out, qc, kc, rows)
    kept.wait()


def last_and_attention(index, chunk, wq, wk, wv, acc, ready, grad_out, tables, normed_all, part):
    _, width = chunk.shape
    total = wq.shape[1] + 2 * wk.shape[1]
    length = grad_out.shape[0]
    extra = [] if acc is None else [acc]
    inputs = 7 + len(extra) + len(ready)
    return pl.pallas_call(
        functools.partial(last_kernel, part, len(ready)),
        out_shape=[
            jax.ShapeDtypeStruct((length, total), bf16),
            jax.ShapeDtypeStruct(normed_all.shape, bf16),
        ],
        in_specs=[smem()] + [whole()] * (inputs - 1) + [anywhere()],
        out_specs=[whole(), anywhere()],
        input_output_aliases={inputs: 1},
        scratch_shapes=[VMEM((length, total), bf16), pltpu.SemaphoreType.DMA],
        compiler_params=params(24),
        cost_estimate=cost(4e9, width * total * 2),
        name="attention",
    )(index, chunk, wq, wk, wv, *extra, *ready, grad_out, tables, far(normed_all))


def back_kernel(part, n, index_ref, grads, wq, wk, wv, gain, normed_all, *rest):
    gain_in = rest[0] if part else None
    outs = rest[-(n + 4) : -4]
    gain_out, scratch, normed, sem = rest[-4:]
    rows, width = outs[0].shape
    qc, kc = wq.shape[1], wk.shape[1]
    copy = pltpu.make_async_copy(
        normed_all.at[:, pl.ds(part * width, width)], normed, sem
    )
    copy.start()
    nt = (((1,), (1,)), ((), ()))
    block = step_size(width, 768)
    for s in range(width // block):
        at = slice(part * width + s * block, part * width + (s + 1) * block)
        value = lax.dot_general(grads[:, :qc], wq[at, :], nt, preferred_element_type=f32)
        value += lax.dot_general(grads[:, qc : qc + kc], wk[at, :], nt, preferred_element_type=f32)
        value += lax.dot_general(grads[:, qc + kc :], wv[at, :], nt, preferred_element_type=f32)
        scratch[:, s * block : (s + 1) * block] = value.astype(bf16)
    for d, out in enumerate(outs):
        owner = lax.rem(index_ref[0] + d, n)
        out[...] = scratch[pl.ds(pl.multiple_of(owner * rows, rows), rows), :]
    copy.wait()
    product = scratch[...].astype(f32) * normed[...].astype(f32)
    if part:
        gain_out[:, : part * width] = gain_in[...]
    at = slice(part * width, (part + 1) * width)
    gain_out[:, at] = jnp.sum(product, axis=0, keepdims=True) / gain[:, at]


def back(index, grads, wq, wk, wv, gain, normed_all, gain_in, n, part, width):
    length, total = grads.shape
    rows = length // n
    extra = [gain_in] if part else []
    return pl.pallas_call(
        functools.partial(back_kernel, part, n),
        out_shape=[jax.ShapeDtypeStruct((rows, width), bf16)] * n
        + [jax.ShapeDtypeStruct((1, (part + 1) * width), f32)],
        in_specs=[smem()] + [whole()] * 5 + [anywhere()] + [whole()] * len(extra),
        out_specs=[whole()] * (n + 1),
        scratch_shapes=[
            VMEM((length, width), bf16),
            VMEM((length, width), bf16),
            pltpu.SemaphoreType.DMA,
        ],
        compiler_params=params(24),
        cost_estimate=cost(2 * length * width * total, width * total * 2),
        name="back_projection",
    )(index, grads, wq, wk, wv, gain, far(normed_all), *extra)


def weight_kernel(qc, kc, block, grads, normed_all, gq, gk, gv, normed, bq, bk, bv, in_sems, sems):
    steps = normed_all.shape[1] // block
    reads = []
    for s in range(steps):
        at = pl.ds(s * block, block)
        copy = pltpu.make_async_copy(normed_all.at[:, at], normed.at[:, at], in_sems.at[s])
        copy.start()
        reads.append(copy)
    tn = (((0,), (0,)), ((), ()))
    columns = (slice(0, qc), slice(qc, qc + kc), slice(qc + kc, qc + 2 * kc))
    writes = []
    for s in range(steps):
        reads[s].wait()
        x = normed[:, s * block : (s + 1) * block]
        at = pl.ds(s * block, block)
        for i, (buffer, out) in enumerate(zip((bq, bk, bv), (gq, gk, gv))):
            value = lax.dot_general(x, grads[:, columns[i]], tn, preferred_element_type=f32)
            buffer[s * block : (s + 1) * block, :] = value.astype(bf16)
            copy = pltpu.make_async_copy(buffer.at[at], out.at[at], sems.at[s * 3 + i])
            copy.start()
            writes.append(copy)
    for copy in writes:
        copy.wait()


def weights(grads, normed_all, qc, kc):
    length, total = grads.shape
    full = normed_all.shape[1]
    block = step_size(full, WEIGHT_ROWS)
    steps = full // block
    shapes = [(full, qc), (full, kc), (full, kc)]
    return pl.pallas_call(
        functools.partial(weight_kernel, qc, kc, block),
        out_shape=[jax.ShapeDtypeStruct(s, bf16) for s in shapes],
        in_specs=[whole(), anywhere()],
        out_specs=[anywhere()] * 3,
        scratch_shapes=[VMEM((length, full), bf16)]
        + [VMEM(s, bf16) for s in shapes]
        + [pltpu.SemaphoreType.DMA((steps,)), pltpu.SemaphoreType.DMA((steps * 3,))],
        compiler_params=params(24),
        cost_estimate=cost(2 * length * full * total, full * total * 2),
        name="weight_gradients",
    )(grads, far(normed_all))


def token_kernel(n, chunks, x_ref, gain_ref, *refs):
    terms, gains, (out, gain_out) = refs[: n * chunks], refs[n * chunks : -2], refs[-2:]
    gain_out[...] = sum(g[...] for g in gains)
    x = x_ref[...].astype(f32)
    inverse = lax.rsqrt(jnp.mean(x * x, axis=-1, keepdims=True) + epsilon)
    width = terms[0].shape[1]
    mean = 0.0
    for c in range(chunks):
        cols = slice(c * width, (c + 1) * width)
        summed = sum(terms[d * chunks + c][...].astype(f32) for d in range(n))
        scaled = summed * gain_ref[:, cols]
        mean += jnp.sum(scaled * (x[:, cols] * inverse), axis=-1, keepdims=True)
    mean = mean / (width * chunks)
    for c in range(chunks):
        cols = slice(c * width, (c + 1) * width)
        summed = sum(terms[d * chunks + c][...].astype(f32) for d in range(n))
        scaled = summed * gain_ref[:, cols]
        out[:, cols] = (inverse * (scaled - (x[:, cols] * inverse) * mean)).astype(bf16)


def token_gradient(x, gain, terms, gains, n, chunks):
    rows, width = x.shape
    block = rows // 4 if rows % 64 == 0 else rows
    by_rows = lambda c: pl.BlockSpec((block, c), lambda s: (s, 0))
    fixed = pl.BlockSpec((1, width), lambda s: (0, 0))
    return pl.pallas_call(
        functools.partial(token_kernel, n, chunks),
        grid=(rows // block,),
        out_shape=[jax.ShapeDtypeStruct(x.shape, bf16), jax.ShapeDtypeStruct(gain.shape, f32)],
        in_specs=[by_rows(width), fixed] + [by_rows(width // chunks)] * len(terms) + [fixed] * n,
        out_specs=[by_rows(width), fixed],
        compiler_params=params(12),
        cost_estimate=cost(1e9, x.size * 8),
        name="token_gradient",
    )(far(x), far(gain), *terms, *gains)


def grid_of(shape, n):
    rows, width = shape
    across = max(1, 8 * n // rows)
    if n % across or rows % (n // across) or width % (across * 128):
        across = 1
    return n // across, across


def cut(array, n):
    down, across = grid_of(array.shape, n)
    rows, width = array.shape
    pieces = array.reshape(down, rows // down, across, width // across)
    return pieces.transpose(0, 2, 1, 3).reshape(n, rows // down, width // across)


def mean_kernel(across, rep_ref, pieces, ours, out, mine_ref, sem):
    n, high, wide = pieces.shape
    row = pl.multiple_of(rep_ref[0] // across * high, high)
    col = pl.multiple_of(lax.rem(rep_ref[0], across) * wide, wide)
    copy = pltpu.make_async_copy(ours.at[pl.ds(row, high), pl.ds(col, wide)], mine_ref, sem)
    copy.start()
    copy.wait()
    mine = mine_ref[...]
    total = jnp.zeros_like(mine)
    for r in range(n):
        total += mine - pieces[r].astype(f32)
    total = (total / n).astype(out.dtype)
    for r in range(n):
        out[r] = total


def mean_pieces(rep, pieces, ours):
    _, across = grid_of(ours.shape, pieces.shape[0])
    return pl.pallas_call(
        functools.partial(mean_kernel, across),
        out_shape=jax.ShapeDtypeStruct(pieces.shape, bf16),
        in_specs=[smem(), whole(), anywhere()],
        out_specs=whole(),
        scratch_shapes=[VMEM(pieces.shape[1:], f32), pltpu.SemaphoreType.DMA],
        compiler_params=params(8),
        cost_estimate=cost(1e8, pieces.size * 6),
        name="mean_pieces",
    )(rep, pieces, far(ours))


def update_kernel(across, pieces, ours, momentum, new_ours, new_momentum):
    n, high, wide = pieces.shape
    for r in range(n):
        row, col = r // across * high, r % across * wide
        at = slice(row, row + high), slice(col, col + wide)
        mean_delta = pieces[r].astype(f32)
        speed = outer_momentum * momentum[at] + mean_delta
        new_momentum[at] = speed
        new_ours[at] = ours[at] - outer_rate * (mean_delta + outer_momentum * speed)


def update(pieces, ours, momentum):
    _, across = grid_of(ours.shape, pieces.shape[0])
    return pl.pallas_call(
        functools.partial(update_kernel, across),
        out_shape=[jax.ShapeDtypeStruct(ours.shape, f32)] * 2,
        in_specs=[whole()] * 3,
        out_specs=[whole()] * 2,
        compiler_params=params(8),
        cost_estimate=cost(1e8, ours.size * 20),
        name="update",
    )(pieces, ours, momentum)


def send(piece, pairs):
    return lax.ppermute(piece, "tp", pairs)


def step(
    tokens,
    norm_gain,
    w_query,
    key_weight,
    value_weight,
    attention_gradient,
    global_fragment,
    momentum,
    local_fragment,
):
    x, wq, wk, wv = tokens[0], w_query[0], key_weight[0], value_weight[0]
    grad_out = attention_gradient[0]
    n, replicas = lax.axis_size("tp"), lax.axis_size("rep")
    here = lax.axis_index("tp")
    index = here.reshape(1).astype(jnp.int32)
    rows, features = x.shape
    qc, kc = wq.shape[1], wk.shape[1]
    chunks = chunk_count(features)
    width = features // chunks
    shift = lambda d: [(j, (j + d) % n) for j in range(n)]

    own = list(norm(x, norm_gain, chunks))
    arrived = [[send(piece, shift(d)) for piece in own] for d in range(1, n)]

    tables = rope_tables(rows * n, HEAD_SIZE)
    own_rows, normed_all = project_own(index, own, wq, wk, wv, tables)
    ready = [own_rows]

    rep = lax.axis_index("rep").reshape(1).astype(jnp.int32)
    pieces = lax.all_to_all(cut(local_fragment[0], replicas), "rep", 0, 0, tiled=False)
    spread = mean_pieces(rep, pieces, global_fragment)

    for d in range(1, n):
        acc = None
        owner = lax.rem(index + (n - d), n)
        for c in range(chunks if d < n - 1 else chunks - 1):
            acc, normed_all = project_part(owner, arrived[d - 1][c], wq, wk, wv, acc, normed_all, c)
        if d < n - 1:
            turn = lax.dynamic_slice_in_dim(tables, owner[0] * rows, rows, 0)
            ready.append(finish(acc, turn, qc, kc))
    last = arrived[n - 2][chunks - 1]
    grads, normed_all = last_and_attention(
        index, last, wq, wk, wv, acc, ready, grad_out, tables, normed_all, chunks - 1
    )

    terms, gain_part = [], None
    for c in range(chunks):
        *pieces_of, gain_part = back(
            index, grads, wq, wk, wv, norm_gain, normed_all, gain_part, n, c, width
        )
        terms.append(pieces_of)
    landed = [[send(terms[c][d], shift(d)) for c in range(chunks)] for d in range(1, n)]
    own_terms = [terms[c][0] for c in range(chunks)]
    gains = [gain_part] + [send(gain_part, shift(d)) for d in range(1, n)]
    grad_wq, grad_wk, grad_wv = weights(grads, normed_all, qc, kc)

    gathered = lax.all_to_all(spread, "rep", 0, 0, tiled=False)
    new_global, new_momentum = update(gathered, global_fragment, momentum)

    grad_tokens, gain_total = token_gradient(
        x, norm_gain, own_terms + [c for group in landed for c in group], gains, n, chunks
    )
    return (
        grad_wq[None],
        grad_wk[None],
        grad_wv[None],
        gain_total,
        grad_tokens[None],
        new_global,
        new_momentum,
    )


def finish_kernel(qc, kc, acc, tables, out):
    parts = acc[:, :qc], acc[:, qc : qc + kc], acc[:, qc + kc :]
    finish_projection(parts, tables[...], out, 0)


def finish(acc, tables, qc, kc):
    return pl.pallas_call(
        functools.partial(finish_kernel, qc, kc),
        out_shape=jax.ShapeDtypeStruct(acc.shape, bf16),
        in_specs=[whole()] * 2,
        out_specs=whole(),
        compiler_params=params(8),
        cost_estimate=cost(1e8, acc.size * 6),
        name="finish_projection",
    )(acc, tables)


def solution(mesh):
    placed = (
        P("rep", "tp", None),
        P("rep", None),
        P("rep", None, "tp"),
        P("rep", None, "tp"),
        P("rep", None, "tp"),
        P("rep", None, "tp"),
        P("tp", None),
        P("tp", None),
        P("rep", "tp", None),
    )
    return jax.shard_map(
        step,
        mesh=mesh,
        in_specs=placed,
        out_specs=(
            P("rep", None, "tp"),
            P("rep", None, "tp"),
            P("rep", None, "tp"),
            P("rep", None),
            P("rep", "tp", None),
            P("tp", None),
            P("tp", None),
        ),
        check_vma=False,
    )
```

```python
import functools
import math

import jax
import jax.numpy as jnp
import numpy as np
from jax import lax
from jax.experimental import pallas as pl
from jax.experimental.pallas import tpu as pltpu
from jax.sharding import PartitionSpec as P


HEAD_SIZE = 128

epsilon = 1e-05
rope_base = 500000.0
outer_rate = 0.7
outer_momentum = 0.9

VMEM = pltpu.VMEM
f32, bf16 = jnp.float32, jnp.bfloat16

WEIGHT_ROWS = 768
TOKEN_STEPS = 2


def whole():
    return pl.BlockSpec(memory_space=VMEM)


def anywhere():
    return pl.BlockSpec(memory_space=pl.ANY)


def far(array):
    return pltpu.with_memory_space_constraint(array, pltpu.HBM)


def smem():
    return pl.BlockSpec(memory_space=pltpu.SMEM)


def params(mib):
    return pltpu.CompilerParams(vmem_limit_bytes=mib << 20)


def cost(flops, nbytes):
    return pl.CostEstimate(flops=int(flops), bytes_accessed=int(nbytes), transcendentals=0)


def rope_tables(length, width):
    middle = width // 2
    frequency = rope_base ** (-2.0 * np.arange(middle) / width)
    angles = np.arange(length)[:, None] * frequency[None, :]
    cosine, sine = np.cos(angles), np.sin(angles)
    tables = (cosine, cosine, -sine, sine)
    return jnp.asarray(np.concatenate(tables, 1).astype(np.float32))


def rope(v, cosine, sine):
    return v * cosine + pltpu.roll(v, v.shape[-1] // 2, 1) * sine


def unrope(v, cosine, sine):
    return v * cosine - pltpu.roll(v, v.shape[-1] // 2, 1) * sine


def chunk_widths(width, thirds):
    first = width * thirds // 3 // 128 * 128
    return (first, width - first) if first else (width,)


def step_size(width, most):
    for n in range(most, 0, -128):
        if width % n == 0:
            return n
    return width


def norm_kernel(x_ref, gain_ref, *outs):
    x = x_ref[...].astype(f32)
    inverse = lax.rsqrt(jnp.mean(x * x, axis=-1, keepdims=True) + epsilon)
    normed = ((x * inverse) * gain_ref[...]).astype(bf16)
    at = 0
    for out in outs:
        out[...] = normed[:, at : at + out.shape[1]]
        at += out.shape[1]


def norm(x, gain, widths):
    rows = x.shape[0]
    return pl.pallas_call(
        norm_kernel,
        out_shape=[jax.ShapeDtypeStruct((rows, w), bf16) for w in widths],
        in_specs=[whole()] * 2,
        out_specs=[whole()] * len(widths),
        compiler_params=params(8),
        cost_estimate=cost(1.0e9, x.size * 4),
        name="norm",
    )(far(x), far(gain))


def project(chunk, wq, wk, wv, rows):
    return [jnp.dot(chunk, w[rows, :], preferred_element_type=f32) for w in (wq, wk, wv)]


def finish_projection(parts, tables, out, row):
    rows = tables.shape[0]
    cosine, sine = tables[:, :HEAD_SIZE], tables[:, HEAD_SIZE:]
    at = 0
    for part, turned in zip(parts, (True, True, False)):
        for h in range(part.shape[1] // HEAD_SIZE):
            piece = part[:, h * HEAD_SIZE : (h + 1) * HEAD_SIZE]
            if turned:
                piece = rope(piece, cosine, sine)
            out[pl.ds(row, rows), at : at + HEAD_SIZE] = piece.astype(bf16)
            at += HEAD_SIZE


def keep(chunk, normed_all, row, at, sem):
    rows, width = chunk.shape
    place = normed_all.at[pl.ds(row, rows), pl.ds(at, width)]
    copy = pltpu.make_async_copy(chunk, place, sem)
    copy.start()
    return copy


def own_kernel(block, depth, index_ref, tables, *refs):
    chunks = refs[:-11]
    wq, wk, wv, out, normed_all, bq, bk, bv, acc, sems, keep_sems = refs[-11:]
    rows = chunks[0].shape[0]
    start = pl.multiple_of(index_ref[0] * rows, rows)
    steps = wq.shape[0] // block
    per_chunk = [ref.shape[1] // block for ref in chunks]
    blocks = [
        (ref, at * block) for ref, count in zip(chunks, per_chunk) for at in range(count)
    ]
    sources, buffers = (wq, wk, wv), (bq, bk, bv)

    def fetch(s):
        part = pl.ds(s * block, block)
        copies = [
            pltpu.make_async_copy(sources[i].at[part], buffers[i].at[part], sems.at[s * 3 + i])
            for i in range(3)
        ]
        for copy in copies:
            copy.start()
        return copies

    flights = [fetch(s) for s in range(depth)]
    kept = [
        keep(ref, normed_all, start, sum(per_chunk[:c]) * block, keep_sems.at[c])
        for c, ref in enumerate(chunks)
    ]
    for s in range(steps):
        for copy in flights[s]:
            copy.wait()
        if s + depth < steps:
            flights.append(fetch(s + depth))
        ref, at = blocks[s]
        parts = project(ref[:, at : at + block], bq, bk, bv, slice(s * block, (s + 1) * block))
        at = 0
        for part in parts:
            cols = slice(at, at + part.shape[1])
            if s == 0:
                acc[:, cols] = part
            else:
                acc[:, cols] += part
            at += part.shape[1]
    qc, kc = wq.shape[1], wk.shape[1]
    parts = acc[:, :qc], acc[:, qc : qc + kc], acc[:, qc + kc :]
    finish_projection(parts, tables[pl.ds(start, rows), :], out, 0)
    for copy in kept:
        copy.wait()


def project_own(index, chunks, wq, wk, wv, tables):
    rows = chunks[0].shape[0]
    qc, kc = wq.shape[1], wk.shape[1]
    block = step_size(math.gcd(*[c.shape[1] for c in chunks]), 512)
    full = wq.shape[0]
    steps = full // block
    total = qc + 2 * kc
    return pl.pallas_call(
        functools.partial(own_kernel, block, min(3, steps)),
        out_shape=[
            jax.ShapeDtypeStruct((rows, total), bf16),
            jax.ShapeDtypeStruct((tables.shape[0], full), bf16),
        ],
        in_specs=[smem(), whole()] + [whole()] * len(chunks) + [anywhere()] * 3,
        out_specs=[whole(), anywhere()],
        scratch_shapes=[
            VMEM((full, qc), bf16),
            VMEM((full, kc), bf16),
            VMEM((full, kc), bf16),
            VMEM((rows, total), f32),
            pltpu.SemaphoreType.DMA((steps * 3,)),
            pltpu.SemaphoreType.DMA((len(chunks),)),
        ],
        compiler_params=params(20),
        cost_estimate=cost(5e9, full * total * 2),
        name="own_projection",
    )(index, tables, *chunks, *[far(w) for w in (wq, wk, wv)])


def part_kernel(offset, row_ref, chunk, wq, wk, wv, *rest):
    out, normed_all, sem = rest[-3:]
    acc_in = rest[0] if len(rest) > 4 else None
    rows, width = chunk.shape
    kept = keep(chunk, normed_all, pl.multiple_of(row_ref[0] * rows, rows), offset, sem)
    at = 0
    for value in project(chunk[...], wq, wk, wv, slice(offset, offset + width)):
        cols = slice(at, at + value.shape[1])
        out[:, cols] = value if acc_in is None else acc_in[:, cols] + value
        at += value.shape[1]
    kept.wait()


def project_part(owner, chunk, wq, wk, wv, acc, normed_all, offset):
    rows, width = chunk.shape
    total = wq.shape[1] + 2 * wk.shape[1]
    extra = [] if acc is None else [acc]
    inputs = 5 + len(extra)
    return pl.pallas_call(
        functools.partial(part_kernel, offset),
        out_shape=[
            jax.ShapeDtypeStruct((rows, total), f32),
            jax.ShapeDtypeStruct(normed_all.shape, bf16),
        ],
        in_specs=[smem()] + [whole()] * (4 + len(extra)) + [anywhere()],
        out_specs=[whole(), anywhere()],
        input_output_aliases={inputs: 1},
        scratch_shapes=[pltpu.SemaphoreType.DMA],
        compiler_params=params(20),
        cost_estimate=cost(2 * rows * width * total, width * total * 2),
        name="part_projection",
    )(owner, chunk, wq, wk, wv, *extra, far(normed_all))


def attention(all_rows, grad_out, tables, out, qc, kc, block):
    length = all_rows.shape[0]
    group = qc // kc
    scale = HEAD_SIZE ** (-0.5)
    nt = (((1,), (1,)), ((), ()))
    tn = (((0,), (0,)), ((), ()))
    key = lax.broadcasted_iota(jnp.int32, (block, block), 0)
    query = lax.broadcasted_iota(jnp.int32, (block, block), 1)
    allowed = jnp.concatenate([key <= query] * group, 1)
    blocks = length // block
    dk, dv = {}, {}

    def head(g, r):
        return slice((g * group + r) * HEAD_SIZE, (g * group + r + 1) * HEAD_SIZE)

    def kcols(g):
        return slice(qc + g * HEAD_SIZE, qc + (g + 1) * HEAD_SIZE)

    def vcols(g):
        return slice(qc + kc + g * HEAD_SIZE, qc + kc + (g + 1) * HEAD_SIZE)

    def opening(g, a):
        rows, keys = slice(a * block, (a + 1) * block), (a + 1) * block
        q = jnp.concatenate([all_rows[rows, head(g, r)] for r in range(group)], 0)
        do = jnp.concatenate([grad_out[rows, head(g, r)] for r in range(group)], 0)
        s = lax.dot_general(all_rows[:keys, kcols(g)], q, nt, preferred_element_type=f32)
        gprob = lax.dot_general(all_rows[:keys, vcols(g)], do, nt, preferred_element_type=f32)
        return g, a, q, do, s, gprob

    def closing(g, a, q, do, s, gprob):
        rows, keys = slice(a * block, (a + 1) * block), (a + 1) * block
        s = s * scale
        corner = jnp.where(allowed, s[keys - block :], -jnp.inf)
        s = corner if a == 0 else jnp.concatenate([s[: keys - block], corner], 0)
        powers = jnp.exp(s - jnp.max(s, axis=0, keepdims=True))
        prob = powers * (1.0 / jnp.sum(powers, axis=0, keepdims=True))
        inner = jnp.sum(gprob * prob, axis=0, keepdims=True)
        low = prob.astype(bf16)
        ds = (prob * (gprob - inner) * scale).astype(bf16)
        part_v = jnp.dot(low, do, preferred_element_type=f32)
        part_k = jnp.dot(ds, q, preferred_element_type=f32)
        dq = lax.dot_general(all_rows[:keys, kcols(g)], ds, tn, preferred_element_type=f32).T
        for b in range(a + 1):
            piece = slice(b * block, (b + 1) * block)
            dv[b] = dv[b] + part_v[piece] if b < a else part_v[piece]
            dk[b] = dk[b] + part_k[piece] if b < a else part_k[piece]
        cosine, sine = tables[rows, :HEAD_SIZE], tables[rows, HEAD_SIZE:]
        for r in range(group):
            piece = unrope(dq[r * block : (r + 1) * block], cosine, sine)
            out[rows, head(g, r)] = piece.astype(bf16)
        if a < blocks - 1:
            return
        for b in range(blocks):
            rows = slice(b * block, (b + 1) * block)
            cosine, sine = tables[rows, :HEAD_SIZE], tables[rows, HEAD_SIZE:]
            out[rows, kcols(g)] = unrope(dk[b], cosine, sine).astype(bf16)
            out[rows, vcols(g)] = dv[b].astype(bf16)

    units = [(g, a) for g in range(kc // HEAD_SIZE) for a in range(blocks)]
    waiting = [opening(*unit) for unit in units[:2]]
    for i in range(len(units)):
        if i + 2 < len(units):
            waiting.append(opening(*units[i + 2]))
        closing(*waiting.pop(0))


def last_kernel(offset, others, index_ref, chunk, wq, wk, wv, *rest):
    extra = len(rest) - (2 * others + 9)
    acc_in = rest[0] if extra else None
    ready = rest[extra : extra + others]
    grad_out, tables, _, out, normed_all, *outs, all_rows, scratch, sem = rest[-(others + 9) :]
    rows, width = chunk.shape
    qc, kc = wq.shape[1], wk.shape[1]
    n = others + 1
    start = pl.multiple_of(lax.rem(index_ref[0] + 1, n) * rows, rows)
    kept = keep(chunk, normed_all, start, offset, sem)
    for d, ref in enumerate(ready):
        owner = lax.rem(index_ref[0] + (n - d), n)
        all_rows[pl.ds(pl.multiple_of(owner * rows, rows), rows), :] = ref[...]
    parts = project(chunk[...], wq, wk, wv, slice(offset, offset + width))
    if acc_in is not None:
        before = acc_in[:, :qc], acc_in[:, qc : qc + kc], acc_in[:, qc + kc :]
        parts = [b + p for b, p in zip(before, parts)]
    finish_projection(parts, tables[pl.ds(start, rows), :], all_rows, start)
    attention(all_rows, grad_out, tables, out, qc, kc, rows)
    spread_back(0, n, index_ref[0], out, wq, wk, wv, outs, scratch)
    kept.wait()


def last_and_attention(index, chunk, wq, wk, wv, acc, ready, grad_out, tables, normed_all, offset, first):
    rows, width = chunk.shape
    total = wq.shape[1] + 2 * wk.shape[1]
    length = grad_out.shape[0]
    extra = [] if acc is None else [acc]
    inputs = 7 + len(extra) + len(ready)
    return pl.pallas_call(
        functools.partial(last_kernel, offset, len(ready)),
        out_shape=[
            jax.ShapeDtypeStruct((length, total), bf16),
            jax.ShapeDtypeStruct(normed_all.shape, bf16),
        ]
        + [jax.ShapeDtypeStruct((rows, first), bf16)] * (len(ready) + 1),
        in_specs=[smem()] + [whole()] * (inputs - 1) + [anywhere()],
        out_specs=[whole(), anywhere()] + [whole()] * (len(ready) + 1),
        input_output_aliases={inputs: 1},
        scratch_shapes=[
            VMEM((length, total), bf16),
            VMEM((length, first), bf16),
            pltpu.SemaphoreType.DMA,
        ],
        compiler_params=params(24),
        cost_estimate=cost(4e9, width * total * 2),
        name="attention",
    )(index, chunk, wq, wk, wv, *extra, *ready, grad_out, tables, far(normed_all))


def spread_back(offset, n, index, grads, wq, wk, wv, outs, scratch):
    rows, width = outs[0].shape
    qc, kc = wq.shape[1], wk.shape[1]
    nt = (((1,), (1,)), ((), ()))
    block = step_size(width, 1024)
    for s in range(width // block):
        at = slice(offset + s * block, offset + (s + 1) * block)
        value = lax.dot_general(grads[:, :qc], wq[at, :], nt, preferred_element_type=f32)
        value += lax.dot_general(grads[:, qc : qc + kc], wk[at, :], nt, preferred_element_type=f32)
        value += lax.dot_general(grads[:, qc + kc :], wv[at, :], nt, preferred_element_type=f32)
        scratch[:, s * block : (s + 1) * block] = value.astype(bf16)
    for d, out in enumerate(outs):
        place = pl.multiple_of(lax.rem(index + d, n) * rows, rows)
        out[...] = scratch[pl.ds(place, rows), :]


def back_kernel(offset, n, index_ref, grads, wq, wk, wv, *rest):
    spread_back(offset, n, index_ref[0], grads, wq, wk, wv, rest[:-1], rest[-1])


def back(index, grads, wq, wk, wv, n, offset, width):
    length, total = grads.shape
    rows = length // n
    return pl.pallas_call(
        functools.partial(back_kernel, offset, n),
        out_shape=[jax.ShapeDtypeStruct((rows, width), bf16)] * n,
        in_specs=[smem()] + [whole()] * 4,
        out_specs=[whole()] * n,
        scratch_shapes=[VMEM((length, width), bf16)],
        compiler_params=params(24),
        cost_estimate=cost(2 * length * width * total, width * total * 2),
        name="back_projection",
    )(index, grads, wq, wk, wv)


def weight_kernel(qc, kc, block, n, widths, index_ref, grads, gain, normed_all, *refs):
    chunks = len(widths)
    terms = refs[: n * chunks]
    gq, gk, gv, gg, normed, turned, bq, bk, bv, in_sems, term_sems, sems = refs[n * chunks :]
    steps = normed_all.shape[1] // block
    reads = []
    for s in range(steps):
        at = pl.ds(s * block, block)
        copy = pltpu.make_async_copy(normed_all.at[:, at], normed.at[:, at], in_sems.at[s])
        copy.start()
        reads.append(copy)
    arrivals = []
    for c, wide in enumerate(widths):
        for d in range(n):
            ref = terms[d * chunks + c]
            rows = ref.shape[0]
            place = pl.multiple_of(lax.rem(index_ref[0] + d, n) * rows, rows)
            into = turned.at[pl.ds(place, rows), pl.ds(sum(widths[:c]), wide)]
            copy = pltpu.make_async_copy(ref, into, term_sems.at[d * chunks + c])
            copy.start()
            arrivals.append(copy)
    tn = (((0,), (0,)), ((), ()))
    columns = (slice(0, qc), slice(qc, qc + kc), slice(qc + kc, qc + 2 * kc))
    writes = []
    for s in range(steps):
        reads[s].wait()
        x = normed[:, s * block : (s + 1) * block]
        at = pl.ds(s * block, block)
        for i, (buffer, out) in enumerate(zip((bq, bk, bv), (gq, gk, gv))):
            value = lax.dot_general(x, grads[:, columns[i]], tn, preferred_element_type=f32)
            buffer[s * block : (s + 1) * block, :] = value.astype(bf16)
            copy = pltpu.make_async_copy(buffer.at[at], out.at[at], sems.at[s * 3 + i])
            copy.start()
            writes.append(copy)
    for copy in arrivals:
        copy.wait()
    for s in range(steps):
        at = slice(s * block, (s + 1) * block)
        product = normed[:, at].astype(f32) * turned[:, at].astype(f32)
        gg[:, at] = jnp.sum(product, axis=0, keepdims=True) / gain[:, at]
    for copy in writes:
        copy.wait()


def weights(index, grads, gain, normed_all, terms, qc, kc, n, widths):
    length, total = grads.shape
    full = normed_all.shape[1]
    block = step_size(full, WEIGHT_ROWS)
    steps = full // block
    shapes = [(full, qc), (full, kc), (full, kc)]
    return pl.pallas_call(
        functools.partial(weight_kernel, qc, kc, block, n, widths),
        out_shape=[jax.ShapeDtypeStruct(s, bf16) for s in shapes]
        + [jax.ShapeDtypeStruct((1, full), f32)],
        in_specs=[smem(), whole(), whole()] + [anywhere()] * (1 + len(terms)),
        out_specs=[anywhere()] * 3 + [whole()],
        scratch_shapes=[VMEM((length, full), bf16)] * 2
        + [VMEM(s, bf16) for s in shapes]
        + [
            pltpu.SemaphoreType.DMA((steps,)),
            pltpu.SemaphoreType.DMA((len(terms),)),
            pltpu.SemaphoreType.DMA((steps * 3,)),
        ],
        compiler_params=params(26),
        cost_estimate=cost(2 * length * full * total, full * total * 2),
        name="weight_gradients",
    )(index, grads, far(gain), far(normed_all), *[far(t) for t in terms])


def token_kernel(n, widths, x_ref, gain_ref, *refs):
    chunks = len(widths)
    terms, out = refs[:-1], refs[-1]
    x = x_ref[...].astype(f32)
    inverse = lax.rsqrt(jnp.mean(x * x, axis=-1, keepdims=True) + epsilon)
    xhat = x * inverse
    scaled, at = [], 0
    for c, wide in enumerate(widths):
        summed = sum(terms[d * chunks + c][...].astype(f32) for d in range(n))
        scaled.append(summed * gain_ref[:, at : at + wide])
        at += wide
    scaled = jnp.concatenate(scaled, 1)
    mean = jnp.mean(scaled * xhat, axis=-1, keepdims=True)
    out[...] = (inverse * (scaled - xhat * mean)).astype(bf16)


def token_gradient(x, gain, terms, n, widths):
    rows, width = x.shape
    block = rows // TOKEN_STEPS if rows % (16 * TOKEN_STEPS) == 0 else rows
    by_rows = lambda c: pl.BlockSpec((block, c), lambda s: (s, 0))
    fixed = pl.BlockSpec((1, width), lambda s: (0, 0))
    return pl.pallas_call(
        functools.partial(token_kernel, n, widths),
        grid=(rows // block,),
        out_shape=jax.ShapeDtypeStruct(x.shape, bf16),
        in_specs=[by_rows(width), fixed] + [by_rows(w) for w in widths] * n,
        out_specs=by_rows(width),
        compiler_params=params(16),
        cost_estimate=cost(1e9, x.size * 8),
        name="token_gradient",
    )(far(x), far(gain), *terms)


def grid_of(shape, n):
    rows, width = shape
    across = max(1, 8 * n // rows)
    if n % across or rows % (n // across) or width % (across * 128):
        across = 1
    return n // across, across


def cut(array, n):
    down, across = grid_of(array.shape, n)
    rows, width = array.shape
    pieces = array.reshape(down, rows // down, across, width // across)
    return pieces.transpose(0, 2, 1, 3).reshape(n, rows // down, width // across)


def mean_kernel(across, rep_ref, pieces, ours, out, mine_ref, sem):
    n, high, wide = pieces.shape
    row = pl.multiple_of(rep_ref[0] // across * high, high)
    col = pl.multiple_of(lax.rem(rep_ref[0], across) * wide, wide)
    copy = pltpu.make_async_copy(ours.at[pl.ds(row, high), pl.ds(col, wide)], mine_ref, sem)
    copy.start()
    total = jnp.zeros(mine_ref.shape, f32)
    for r in range(n):
        total += pieces[r].astype(f32)
    copy.wait()
    total = (mine_ref[...] - total / n).astype(out.dtype)
    for r in range(n):
        out[r] = total


def mean_pieces(rep, pieces, ours):
    _, across = grid_of(ours.shape, pieces.shape[0])
    return pl.pallas_call(
        functools.partial(mean_kernel, across),
        out_shape=jax.ShapeDtypeStruct(pieces.shape, bf16),
        in_specs=[smem(), whole(), anywhere()],
        out_specs=whole(),
        scratch_shapes=[VMEM(pieces.shape[1:], f32), pltpu.SemaphoreType.DMA],
        compiler_params=params(8),
        cost_estimate=cost(1e8, pieces.size * 6),
        name="mean_pieces",
    )(rep, pieces, far(ours))


def update_kernel(across, pieces, ours, momentum, *rest):
    *gains, new_ours, new_momentum, gain_out = rest
    gain_out[...] = sum(g[...] for g in gains)
    n, high, wide = pieces.shape
    for r in range(n):
        row, col = r // across * high, r % across * wide
        at = slice(row, row + high), slice(col, col + wide)
        mean_delta = pieces[r].astype(f32)
        speed = outer_momentum * momentum[at] + mean_delta
        new_momentum[at] = speed
        new_ours[at] = ours[at] - outer_rate * (mean_delta + outer_momentum * speed)


def update(pieces, ours, momentum, gains):
    _, across = grid_of(ours.shape, pieces.shape[0])
    shapes = [ours.shape, ours.shape, gains[0].shape]
    return pl.pallas_call(
        functools.partial(update_kernel, across),
        out_shape=[jax.ShapeDtypeStruct(s, f32) for s in shapes],
        in_specs=[whole()] * (3 + len(gains)),
        out_specs=[whole()] * 3,
        compiler_params=params(8),
        cost_estimate=cost(1e8, ours.size * 20),
        name="update",
    )(pieces, ours, momentum, *gains)


def send(piece, pairs):
    return lax.ppermute(piece, "tp", pairs)


def step(
    tokens,
    norm_gain,
    w_query,
    key_weight,
    value_weight,
    attention_gradient,
    global_fragment,
    momentum,
    local_fragment,
):
    x, wq, wk, wv = tokens[0], w_query[0], key_weight[0], value_weight[0]
    grad_out = attention_gradient[0]
    n, replicas = lax.axis_size("tp"), lax.axis_size("rep")
    here = lax.axis_index("tp")
    index = here.reshape(1).astype(jnp.int32)
    rows, features = x.shape
    qc, kc = wq.shape[1], wk.shape[1]
    parts, widths = chunk_widths(features, 2), chunk_widths(features, 1)
    chunks = len(widths)
    shift = lambda d: [(j, (j + d) % n) for j in range(n)]

    own = list(norm(x, norm_gain, parts))
    arrived = [[send(piece, shift(d)) for piece in own] for d in range(1, n)]

    tables = rope_tables(rows * n, HEAD_SIZE)
    own_rows, normed_all = project_own(index, own, wq, wk, wv, tables)
    ready = [own_rows]

    rep = lax.axis_index("rep").reshape(1).astype(jnp.int32)
    pieces = lax.all_to_all(cut(local_fragment[0], replicas), "rep", 0, 0, tiled=False)
    spread = mean_pieces(rep, pieces, global_fragment)

    offsets = [sum(parts[:c]) for c in range(chunks)]
    for d in range(1, n):
        acc = None
        owner = lax.rem(index + (n - d), n)
        for c in range(chunks if d < n - 1 else chunks - 1):
            acc, normed_all = project_part(
                owner, arrived[d - 1][c], wq, wk, wv, acc, normed_all, offsets[c]
            )
        if d < n - 1:
            turn = lax.dynamic_slice_in_dim(tables, owner[0] * rows, rows, 0)
            ready.append(finish(acc, turn, qc, kc))
    last = arrived[n - 2][chunks - 1]
    grads, normed_all, *terms = last_and_attention(
        index, last, wq, wk, wv, acc, ready, grad_out, tables, normed_all, offsets[-1], widths[0]
    )

    terms = [terms]
    for c in range(1, chunks):
        terms.append(back(index, grads, wq, wk, wv, n, sum(widths[:c]), widths[c]))
    landed = [[send(terms[c][d], shift(d)) for c in range(chunks)] for d in range(1, n)]
    own_terms = [terms[c][0] for c in range(chunks)]
    ordered = [terms[c][d] for d in range(n) for c in range(chunks)]
    grad_wq, grad_wk, grad_wv, gain_part = weights(
        index, grads, norm_gain, normed_all, ordered, qc, kc, n, widths
    )
    gains = [gain_part] + [send(gain_part, shift(d)) for d in range(1, n)]

    gathered = lax.all_to_all(spread, "rep", 0, 0, tiled=False)
    new_global, new_momentum, gain_total = update(gathered, global_fragment, momentum, gains)

    grad_tokens = token_gradient(
        x, norm_gain, own_terms + [c for group in landed for c in group], n, widths
    )
    return (
        grad_wq[None],
        grad_wk[None],
        grad_wv[None],
        gain_total,
        grad_tokens[None],
        new_global,
        new_momentum,
    )


def finish_kernel(qc, kc, acc, tables, out):
    parts = acc[:, :qc], acc[:, qc : qc + kc], acc[:, qc + kc :]
    finish_projection(parts, tables[...], out, 0)


def finish(acc, tables, qc, kc):
    return pl.pallas_call(
        functools.partial(finish_kernel, qc, kc),
        out_shape=jax.ShapeDtypeStruct(acc.shape, bf16),
        in_specs=[whole()] * 2,
        out_specs=whole(),
        compiler_params=params(8),
        cost_estimate=cost(1e8, acc.size * 6),
        name="finish_projection",
    )(acc, tables)


def solution(mesh):
    placed = (
        P("rep", "tp", None),
        P("rep", None),
        P("rep", None, "tp"),
        P("rep", None, "tp"),
        P("rep", None, "tp"),
        P("rep", None, "tp"),
        P("tp", None),
        P("tp", None),
        P("rep", "tp", None),
    )
    return jax.shard_map(
        step,
        mesh=mesh,
        in_specs=placed,
        out_specs=(
            P("rep", None, "tp"),
            P("rep", None, "tp"),
            P("rep", None, "tp"),
            P("rep", None),
            P("rep", "tp", None),
            P("tp", None),
            P("tp", None),
        ),
        check_vma=False,
    )
```
